32 devices in a mesh: dp: 8 (over z, x), tensor: 4 (over y, core).
Axes of the slice: x: 2, y: 2, z: 4, core: 2. Of those that a mesh axis runs over, the one named last changes fastest.
Arguments:
- streams: bfloat16 [128, 4, 7168], P('dp', None, 'tensor'), may hold values from -12 to 12
- mix_weight: bfloat16 [24, 4, 7168], P(None, None, 'tensor'), may hold values from -0.0625 to 0.0625
- mix_bias: float32 [24], replicated, may hold values from -4 to 4
- gate_weight: bfloat16 [18432, 7168], P('dp', 'tensor'), may hold values from -0.0625 to 0.0625
- up_weight: bfloat16 [18432, 7168], P('dp', 'tensor'), may hold values from -0.0625 to 0.0625
- down_weight: bfloat16 [18432, 7168], P('dp', 'tensor'), may hold values from -0.046875 to 0.046875
Outputs:
- new_streams: bfloat16 [128, 4, 7168], P('dp', None, 'tensor')
The draws below stay inside these ranges and needn't reach their ends.
All inputs are finite; a program needn't handle non-finite values.
Results may differ from the reference program's by a relative error of at most 0.006.
The reference program's roundings to bfloat16 on the way (of `mlp_input` and `hidden`) count: a program that leaves them out, or rounds other values in their place, can miss the bound.
Values may be sent and summed in bfloat16 or wider, within the bound.
A program may use at most 64 MiB of HBM per device.

```python
import jax
import jax.numpy as jnp
from jax import lax

D = 7168
FF = 18432
STREAMS = 4
ITERS = 20
LOGITS = 24
TOKENS = 128


def draw_streams(key, part):
    normal_part = jax.random.normal(jax.random.fold_in(key, 11), (TOKENS, STREAMS, D), jnp.float32)
    return jnp.clip(normal_part, -12.0, 12.0).astype(jnp.bfloat16)


def block_scale(own_key, dims, split, low, high):
    level, own = 1.0, jax.random.fold_in(own_key, 6)
    for axis_at, shards_of in split:
        steps = jnp.exp(jax.random.uniform(jax.random.fold_in(own, axis_at), (shards_of,), jnp.float32, low / len(split), high / len(split)))
        level = level * jnp.repeat(steps, dims[axis_at] // shards_of).reshape([-1 if axis == axis_at else 1 for axis in range(len(dims))])
    return level


def gaussian(key, dims, width, limit, shards=(), held_as=jnp.bfloat16):
    entries = width * jax.random.normal(key, dims, jnp.float32)
    if shards:
        entries = entries * block_scale(key, dims, shards, -0.22, 0.18)
    return jnp.clip(entries, -limit, limit).astype(held_as)


def setup_inputs(seed: int = 0) -> dict:
    splits = jax.random.split(jax.random.key(seed), 7)
    streams = draw_streams(jax.random.fold_in(splits[6], 71), 0)
    mix_weight = gaussian(splits[1], (LOGITS, STREAMS, D), (2.0 / (STREAMS * D) ** 0.5), 0.0625, ((2, 4),))
    mix_bias = gaussian(splits[2], (LOGITS,), 1.0, 4.0, (), jnp.float32)
    gate_weight = gaussian(splits[3], (FF, D), D ** -0.5, 0.0625, ((0, 8), (1, 4)))
    up_weight = gaussian(splits[4], (FF, D), D ** -0.5, 0.0625, ((0, 8), (1, 4)))
    down_weight = gaussian(splits[5], (FF, D), FF ** -0.5, 0.046875, ((0, 8), (1, 4)))
    return {"streams": streams, "mix_weight": mix_weight, "mix_bias": mix_bias, "gate_weight": gate_weight, "up_weight": up_weight, "down_weight": down_weight}


epsilon = 1e-06

def normalize(sweep_index, matrix):
    matrix = matrix / lax.optimization_barrier(jnp.sum(matrix, axis=2, keepdims=True))
    return matrix / lax.optimization_barrier(jnp.sum(matrix, axis=1, keepdims=True))

def mixing(raw_logits, squares, mix_bias):
    scale_inv = lax.rsqrt(squares / (STREAMS * D) + epsilon)
    logits = raw_logits * scale_inv[:, None] + mix_bias[None, :]
    pre_gate = jax.nn.sigmoid(logits[:, :STREAMS])
    post_gate = 2.0 * jax.nn.sigmoid(logits[:, STREAMS:2 * STREAMS])
    matrix = jnp.exp(logits[:, 2 * STREAMS:]).reshape(-1, STREAMS, STREAMS)
    matrix = lax.fori_loop(0, ITERS, normalize, matrix)
    return (pre_gate, post_gate, matrix)

def reference(streams, mix_weight, mix_bias, gate_weight, up_weight, down_weight):
    row_count = streams.shape[0]
    flat_rows = streams.reshape(row_count, STREAMS * D)
    raw_logits = jnp.dot(flat_rows, mix_weight.reshape(LOGITS, STREAMS * D).T, preferred_element_type=jnp.float32)
    stream_wide = streams.astype(jnp.float32)
    squares = lax.optimization_barrier(jnp.sum(stream_wide * stream_wide, axis=(1, 2)))
    pre_gate, post_gate, res_mix = mixing(raw_logits, squares, mix_bias)
    mlp_input = jnp.einsum('ts,tsc->tc', pre_gate, stream_wide, precision=lax.Precision.HIGHEST).astype(jnp.bfloat16)
    gate = jnp.dot(mlp_input, gate_weight.T, preferred_element_type=jnp.float32)
    up_part = jnp.dot(mlp_input, up_weight.T, preferred_element_type=jnp.float32)
    hidden = (jax.nn.silu(gate) * up_part).astype(jnp.bfloat16)
    mlp_out = jnp.dot(hidden, down_weight, preferred_element_type=jnp.float32)
    mixed = jnp.einsum('tij,tjc->tic', res_mix, stream_wide, precision=lax.Precision.HIGHEST)
    mixed = mixed + post_gate[:, :, None] * mlp_out[:, None, :]
    return mixed.astype(jnp.bfloat16)
```

```python
import functools
import math

import jax
import jax.numpy as jnp
from jax import lax
from jax.experimental import pallas as pl
from jax.experimental.pallas import tpu as pltpu
from jax.sharding import PartitionSpec as P

D = 7168
ITERS = 20


epsilon = 1e-06


def normalize(sweep_index, matrix):
    matrix = matrix / jnp.sum(matrix, axis=2, keepdims=True)
    return matrix / jnp.sum(matrix, axis=1, keepdims=True)


def mixing(raw_logits, squares, mix_bias, stream_count):
    scale_inv = lax.rsqrt(squares / (stream_count * D) + epsilon)
    logits = raw_logits * scale_inv[:, None] + mix_bias[None, :]
    pre_gate = jax.nn.sigmoid(logits[:, :stream_count])
    post_gate = 2.0 * jax.nn.sigmoid(logits[:, stream_count : 2 * stream_count])
    matrix = jnp.exp(logits[:, 2 * stream_count :]).reshape(-1, stream_count, stream_count)
    matrix = lax.fori_loop(0, ITERS, normalize, matrix)
    return (pre_gate, post_gate, matrix)


def contract_last(weights, rows):
    return lax.dot_general(
        weights, rows, (((1,), (1,)), ((), ())), preferred_element_type=jnp.float32
    )


def per_device(streams, mix_weight, mix_bias, gate_weight, up_weight, down_weight):
    tok_rows, stream_count, width_local = streams.shape
    logit_count = mix_weight.shape[0]
    flat_rows = streams.reshape(tok_rows, stream_count * width_local)
    flat_weight = mix_weight.reshape(logit_count, stream_count * width_local)
    raw_logits = lax.dot_general(
        flat_rows, flat_weight, (((1,), (1,)), ((), ())), preferred_element_type=jnp.float32
    )
    stream_wide = streams.astype(jnp.float32)
    squares = jnp.sum(stream_wide * stream_wide, axis=(1, 2))
    total_logits, total_squares = lax.psum((raw_logits, squares), "tensor")
    pre_gate, post_gate, res_mix = mixing(total_logits, total_squares, mix_bias, stream_count)
    mlp_input = jnp.einsum(
        "ts,tsc->tc", pre_gate, stream_wide, precision=lax.Precision.HIGHEST
    ).astype(jnp.bfloat16)
    unit_local = gate_weight.shape[0]
    block_rows = lax.all_gather(mlp_input, "dp", axis=0, tiled=True)
    gate_part = contract_last(gate_weight, block_rows)
    up_part = contract_last(up_weight, block_rows)
    both_parts = jnp.concatenate((gate_part, up_part), axis=0)
    unit_share = lax.psum_scatter(both_parts, "tensor", scatter_dimension=1, tiled=True)
    hidden_share = (jax.nn.silu(unit_share[:unit_local]) * unit_share[unit_local:]).astype(
        jnp.bfloat16
    )
    hidden = lax.all_gather(hidden_share, "tensor", axis=1, tiled=True)
    mlp_out = lax.psum_scatter(
        lax.dot_general(
            hidden, down_weight, (((0,), (0,)), ((), ())), preferred_element_type=jnp.float32
        ),
        "dp",
        scatter_dimension=0,
        tiled=True,
    )
    mixed = jnp.einsum("tij,tjc->tic", res_mix, stream_wide, precision=lax.Precision.HIGHEST)
    mixed = mixed + post_gate[:, :, None] * mlp_out[:, None, :]
    return mixed.astype(jnp.bfloat16)


MESH = pl.DeviceIdType.MESH
UNIT_CHUNK = 256
COLUMN_CHUNK = 256
PAIR = 2
VMEM_BUDGET = 58 * 1024 * 1024


def column(values, at):
    return values[:, at : at + 1]


def sigmoid(v):
    return 1.0 / (1.0 + jnp.exp(-v))


def layer_kernel(
    plan,
    s_ref,
    mw_ref,
    bias_ref,
    gate_hbm,
    up_hbm,
    down_hbm,
    out_ref,
    gate_v,
    up_v,
    down_v,
    part,
    part_in,
    post,
    rows_all,
    mixed,
    sums,
    pair_out,
    pair_in,
    pair_sum,
    ring_out,
    ring_in,
    hidden,
    prod,
    cross_out,
    cross_in,
    cross_sum,
    line_out,
    line_in,
    w_sem,
    a_send,
    a_recv,
    bz_send,
    bz_recv,
    bx_send,
    bx_recv,
    c1_send,
    c1_recv,
    c2_send,
    c2_recv,
    c3_send,
    c3_recv,
    c4_send,
    c4_recv,
    d1_send,
    d1_recv,
    d2_send,
    d2_recv,
):
    zs, ys, tensors, chunks, nc, columns, cc, width_all = plan
    streams, tok, width = s_ref.shape
    dp = lax.axis_index("dp")
    tp = lax.axis_index("tensor")
    z, x = lax.div(dp, PAIR), lax.rem(dp, PAIR)
    y, core = lax.div(tp, PAIR), lax.rem(tp, PAIR)
    x_peer = (z * PAIR + 1 - x, tp)
    core_peer = (dp, y * PAIR + 1 - core)

    def z_at(r):
        return lax.rem(z + r + zs, zs)

    def y_at(r):
        return lax.rem(y + r + ys, ys)

    def z_peer(r):
        return (z_at(r) * PAIR + x, tp)

    def y_peer(r):
        return (dp, y_at(r) * PAIR + core)

    def t_peer(r):
        return (dp, lax.rem(tp + r, tensors))

    def send(src, dst, ssem, rsem, peer):
        return pltpu.make_async_remote_copy(
            src_ref=src, dst_ref=dst, send_sem=ssem, recv_sem=rsem, device_id=peer, device_id_type=MESH
        )

    def weight_copy(k, which):
        hbm, vmem = ((gate_hbm, gate_v), (up_hbm, up_v), (down_hbm, down_v))[which]
        return pltpu.make_async_copy(hbm.at[pl.ds(k * nc, nc)], vmem.at[pl.ds(k * nc, nc)], w_sem.at[which, k])

    def start_gate_up(k, _):
        weight_copy(k, 0).start()
        weight_copy(k, 1).start()
        return 0

    def start_down(k, _):
        weight_copy(k, 2).start()
        return 0

    lax.fori_loop(0, chunks, start_gate_up, 0)
    lax.fori_loop(0, chunks, start_down, 0)

    barrier = pltpu.get_barrier_semaphore()
    peers = [t_peer(r) for r in range(1, tensors)] + [x_peer] + [z_peer(r) for r in range(1, zs)]
    for peer in peers:
        pl.semaphore_signal(barrier, inc=1, device_id=peer, device_id_type=MESH)

    raw = jnp.zeros((tok, mw_ref.shape[1]), jnp.float32)
    squares = jnp.zeros((tok, 1), jnp.float32)
    for j in range(streams):
        raw += contract_last(s_ref[j], mw_ref[j])
        wide = s_ref[j].astype(jnp.float32)
        squares += jnp.sum(wide * wide, axis=1, keepdims=True)
    part[0] = jnp.zeros((tok, part.shape[2]), jnp.float32)
    part[0, :, : raw.shape[1]] = raw
    part[1] = jnp.broadcast_to(squares, (tok, part.shape[2]))
    pl.semaphore_wait(barrier, len(peers))

    def a_copy(r):
        return send(part, part_in.at[r - 1], a_send.at[r - 1], a_recv.at[r - 1], t_peer(r))

    for r in range(1, tensors):
        a_copy(r).start()
    for r in range(1, tensors):
        a_copy(r).wait_recv()
    total = part[...]
    for r in range(1, tensors):
        total = total + part_in[r - 1]
    scale_inv = lax.rsqrt(total[1] / width_all + epsilon)
    logits = total[0] * scale_inv + bias_ref[...]
    gates = sigmoid(logits)
    mlp_input = column(gates, 0) * s_ref[0].astype(jnp.float32)
    for j in range(1, streams):
        mlp_input += column(gates, j) * s_ref[j].astype(jnp.float32)
    rows_all[z] = mlp_input.astype(jnp.bfloat16)

    def bz_copy(r):
        return send(rows_all.at[z], rows_all.at[z], bz_send.at[r - 1], bz_recv.at[r - 1], z_peer(r))

    def bx_copy(r):
        at = z_at(-r)
        return send(rows_all.at[at], rows_all.at[zs + at], bx_send.at[r], bx_recv.at[r], x_peer)

    bx_copy(0).start()
    for r in range(1, zs):
        bz_copy(r).start()
    for i in range(streams):
        post[i] = jnp.broadcast_to(2.0 * column(gates, streams + i), (tok, post.shape[2]))

    entries = jnp.exp(logits)
    mat = tuple(column(entries, 2 * streams + at) for at in range(streams * streams))

    def sweep(_, m):
        m = list(m)
        for i in range(streams):
            total_row = m[i * streams]
            for j in range(1, streams):
                total_row = total_row + m[i * streams + j]
            inv = 1.0 / total_row
            for j in range(streams):
                m[i * streams + j] = m[i * streams + j] * inv
        for j in range(streams):
            total_col = m[j]
            for i in range(1, streams):
                total_col = total_col + m[i * streams + j]
            inv = 1.0 / total_col
            for i in range(streams):
                m[i * streams + j] = m[i * streams + j] * inv
        return tuple(m)

    order = sorted(range(1, zs), key=lambda r: min(r, zs - r))
    for r in order:
        send(rows_all.at[z], rows_all.at[z_at(-r)], bz_send.at[r - 1], bz_recv.at[r - 1], z_peer(r)).wait_recv()
        bx_copy(r).start()
    mat = lax.fori_loop(0, ITERS, sweep, mat)
    for i in range(streams):
        line = mat[i * streams] * s_ref[0].astype(jnp.float32)
        for j in range(1, streams):
            line += mat[i * streams + j] * s_ref[j].astype(jnp.float32)
        mixed[i] = line

    def bx_arrival(r):
        at = z_at(-r)
        return send(rows_all.at[at], rows_all.at[zs + at], bx_send.at[r], bx_recv.at[r], x_peer)

    for r in range(zs):
        bx_arrival(r).wait_recv()

    tokens = PAIR * zs * tok
    half = tokens // PAIR
    quarter = half // ys
    own_slot = core * ys + y

    def c1_copy(k):
        return send(pair_out.at[k], pair_in.at[k], c1_send.at[k], c1_recv.at[k], core_peer)

    def c2_copy(k, r):
        at = (k * (ys - 1)) + r - 1
        return send(ring_out.at[at], ring_in.at[at], c2_send.at[at], c2_recv.at[at], y_peer(r))

    def units(k):
        return pl.ds(pl.multiple_of(k * nc, nc), nc)

    def c3_copy(k, r):
        at = (k * (ys - 1)) + r - 1
        piece = hidden.at[own_slot, :, units(k)]
        return send(piece, piece, c3_send.at[at], c3_recv.at[at], y_peer(r))

    def c3_arrival(k, r):
        at = (k * (ys - 1)) + r - 1
        piece = hidden.at[core * ys + y_at(-r), :, units(k)]
        return send(piece, piece, c3_send.at[at], c3_recv.at[at], y_peer(r))

    def c4_copy(k, r):
        at = k * ys + r
        piece = hidden.at[core * ys + y_at(-r), :, units(k)]
        return send(piece, piece, c4_send.at[at], c4_recv.at[at], core_peer)

    def c4_arrival(k, r):
        at = k * ys + r
        piece = hidden.at[(1 - core) * ys + y_at(-r), :, units(k)]
        return send(piece, piece, c4_send.at[at], c4_recv.at[at], core_peer)

    def c_first(k):
        weight_copy(k, 0).wait()
        weight_copy(k, 1).wait()
        rows = rows_all[...].reshape(tokens, width)
        sums[k, :, :, :nc] = contract_last(rows, gate_v[pl.ds(k * nc, nc)]).reshape(PAIR, half, nc)
        sums[k, :, :, nc:] = contract_last(rows, up_v[pl.ds(k * nc, nc)]).reshape(PAIR, half, nc)
        pair_out[k] = sums[k, 1 - core].astype(jnp.bfloat16)
        c1_copy(k).start()

    def c_second(k):
        c1_copy(k).wait_recv()
        both = sums[k, core] + pair_in[k].astype(jnp.float32)
        pair_sum[k] = both.reshape(ys, quarter, PAIR * nc)
        for r in range(1, ys):
            ring_out[k * (ys - 1) + r - 1] = pair_sum[k, y_at(r)].astype(jnp.bfloat16)
            c2_copy(k, r).start()

    def c_third(k):
        both = pair_sum[k, y]
        for r in range(1, ys):
            c2_copy(k, r).wait_recv()
            both = both + ring_in[k * (ys - 1) + r - 1].astype(jnp.float32)
        gate, up = both[:, :nc], both[:, nc:]
        hidden[own_slot, :, units(k)] = (gate / (1.0 + jnp.exp(-gate)) * up).astype(jnp.bfloat16)
        for r in range(1, ys):
            c3_copy(k, r).start()
        c4_copy(k, 0).start()

    def c_fourth(k):
        for r in range(1, ys):
            c3_arrival(k, r).wait_recv()
            c4_copy(k, r).start()

    def pipeline(count, stages):
        last = max(lag for lag, _ in stages)

        def step(t, _):
            for lag, stage in stages:
                @pl.when(jnp.logical_and(t >= lag, t < count + lag))
                def _():
                    stage(t - lag)

            return 0

        lax.fori_loop(0, count + last, step, 0)

    pipeline(chunks, ((0, c_first), (2, c_second), (4, c_third), (6, c_fourth)))

    def finish_c(k, _):
        for r in range(ys):
            c4_arrival(k, r).wait_recv()
        weight_copy(k, 2).wait()
        return 0

    lax.fori_loop(0, chunks, finish_c, 0)

    def d1_copy(n):
        return send(cross_out.at[n], cross_in.at[n], d1_send.at[n], d1_recv.at[n], x_peer)

    def d2_copy(n, r):
        at = n * (zs - 1) + r - 1
        return send(line_out.at[at], line_in.at[at], d2_send.at[at], d2_recv.at[at], z_peer(r))

    def cols(n):
        return pl.ds(pl.multiple_of(n * cc, cc), cc)

    def d_first(n):
        rows = hidden[...].reshape(tokens, hidden.shape[2])
        product = jnp.dot(rows, down_v[:, cols(n)], preferred_element_type=jnp.float32)
        prod[n] = product[:half]
        cross_out[n] = product[half:].astype(jnp.bfloat16)
        d1_copy(n).start()

    def d_second(n):
        d1_copy(n).wait_recv()
        cross_sum[n] = (prod[n] + cross_in[n].astype(jnp.float32)).reshape(zs, tok, cc)
        for r in range(1, zs):
            line_out[n * (zs - 1) + r - 1] = cross_sum[n, z_at(r)].astype(jnp.bfloat16)
            d2_copy(n, r).start()

    def d_third(n):
        mlp_out = cross_sum[n, z]
        for r in range(1, zs):
            d2_copy(n, r).wait_recv()
            mlp_out = mlp_out + line_in[n * (zs - 1) + r - 1].astype(jnp.float32)
        for i in range(streams):
            out_ref[i, :, cols(n)] = (mixed[i, :, cols(n)] + column(post[i], 0) * mlp_out).astype(jnp.bfloat16)

    pipeline(columns, ((0, d_first), (1, d_second), (3, d_third)))

    for r in range(1, tensors):
        a_copy(r).wait_send()
    for r in range(1, zs):
        bz_copy(r).wait_send()
    for r in range(zs):
        bx_copy(r).wait_send()

    def drain_c(k, _):
        c1_copy(k).wait_send()
        for r in range(1, ys):
            c2_copy(k, r).wait_send()
            c3_copy(k, r).wait_send()
        for r in range(ys):
            c4_copy(k, r).wait_send()
        return 0

    def drain_d(n, _):
        d1_copy(n).wait_send()
        for r in range(1, zs):
            d2_copy(n, r).wait_send()
        return 0

    lax.fori_loop(0, chunks, drain_c, 0)
    lax.fori_loop(0, columns, drain_d, 0)


def layer_scratch(zs, ys, tensors, tok, streams, width, units, nc, cc):
    tokens = PAIR * zs * tok
    half = tokens // PAIR
    quarter = half // ys
    chunks, columns = units // nc, width // cc
    f32, bf16 = jnp.float32, jnp.bfloat16
    lanes = 128
    arrays = [
        ((units, width), bf16),
        ((units, width), bf16),
        ((units, width), bf16),
        ((2, tok, lanes), f32),
        ((tensors - 1, 2, tok, lanes), f32),
        ((streams, tok, lanes), f32),
        ((PAIR * zs, tok, width), bf16),
        ((streams, tok, width), f32),
        ((chunks, PAIR, half, 2 * nc), f32),
        ((chunks, half, 2 * nc), bf16),
        ((chunks, half, 2 * nc), bf16),
        ((chunks, ys, quarter, 2 * nc), f32),
        ((chunks * (ys - 1), quarter, 2 * nc), bf16),
        ((chunks * (ys - 1), quarter, 2 * nc), bf16),
        ((PAIR * ys, quarter, units), bf16),
        ((columns, half, cc), f32),
        ((columns, half, cc), bf16),
        ((columns, half, cc), bf16),
        ((columns, zs, tok, cc), f32),
        ((columns * (zs - 1), tok, cc), bf16),
        ((columns * (zs - 1), tok, cc), bf16),
    ]
    both = lambda count: [(count,), (count,)]
    sems = [(3, chunks)]
    for count in (tensors - 1, zs - 1, zs, chunks, chunks * (ys - 1), chunks * (ys - 1), chunks * ys, columns, columns * (zs - 1)):
        sems += both(count)
    size = sum(math.prod(shape) * jnp.dtype(kind).itemsize for shape, kind in arrays)
    return arrays, sems, size


def fused(mesh, streams, mix_weight, mix_bias, gate_weight, up_weight, down_weight):
    tok, stream_count, width = streams.shape
    units = gate_weight.shape[0]
    dps, tensors = mesh.shape["dp"], mesh.shape["tensor"]
    zs, ys = dps // PAIR, tensors // PAIR
    nc, cc = UNIT_CHUNK, COLUMN_CHUNK
    arrays, sems, _ = layer_scratch(zs, ys, tensors, tok, stream_count, width, units, nc, cc)
    plan = (zs, ys, tensors, units // nc, nc, width // cc, cc, stream_count * width * tensors)
    bias = jnp.pad(mix_bias, (0, 128 - mix_bias.shape[0]))[None, :]
    vmem = pl.BlockSpec(memory_space=pltpu.VMEM)
    hbm = pl.BlockSpec(memory_space=pl.ANY)
    out = pl.pallas_call(
        functools.partial(layer_kernel, plan),
        out_shape=jax.ShapeDtypeStruct((stream_count, tok, width), jnp.bfloat16),
        in_specs=[vmem, vmem, vmem, hbm, hbm, hbm],
        out_specs=vmem,
        scratch_shapes=[pltpu.VMEM(shape, kind) for shape, kind in arrays]
        + [pltpu.SemaphoreType.DMA(shape) for shape in sems],
        compiler_params=pltpu.CompilerParams(
            collective_id=0, has_side_effects=True, vmem_limit_bytes=VMEM_BUDGET
        ),
    )(streams.transpose(1, 0, 2), mix_weight.transpose(1, 0, 2), bias, gate_weight, up_weight, down_weight)
    return out.transpose(1, 0, 2)


def fits(mesh, streams, mix_weight, gate_weight):
    tok, stream_count, width = streams.shape
    units = gate_weight.shape[0]
    dps, tensors = mesh.shape["dp"], mesh.shape["tensor"]
    if dps % PAIR or tensors % PAIR or dps < 2 * PAIR or tensors < 2 * PAIR:
        return False
    zs, ys = dps // PAIR, tensors // PAIR
    if units % UNIT_CHUNK or width % COLUMN_CHUNK or tok % 16 or (zs * tok) % (16 * ys):
        return False
    if mix_weight.shape[0] > 128:
        return False
    size = layer_scratch(zs, ys, tensors, tok, stream_count, width, units, UNIT_CHUNK, COLUMN_CHUNK)[2]
    return size < VMEM_BUDGET * 3 // 4


def solution(mesh):
    in_specs = (
        P("dp", None, "tensor"),
        P(None, None, "tensor"),
        P(),
        P("dp", "tensor"),
        P("dp", "tensor"),
        P("dp", "tensor"),
    )
    out_specs = P("dp", None, "tensor")

    def step(streams, mix_weight, mix_bias, gate_weight, up_weight, down_weight):
        operands = (streams, mix_weight, mix_bias, gate_weight, up_weight, down_weight)
        if fits(mesh, streams, mix_weight, gate_weight):
            return fused(mesh, *operands)
        return per_device(*operands)

    return jax.shard_map(step, mesh=mesh, in_specs=in_specs, out_specs=out_specs, check_vma=False)
```

```python
import functools
import math

import jax
import jax.numpy as jnp
from jax import lax
from jax.experimental import pallas as pl
from jax.experimental.pallas import tpu as pltpu
from jax.sharding import PartitionSpec as P

D = 7168
ITERS = 20


epsilon = 1e-06


def normalize(sweep_index, matrix):
    matrix = matrix / jnp.sum(matrix, axis=2, keepdims=True)
    return matrix / jnp.sum(matrix, axis=1, keepdims=True)


def mixing(raw_logits, squares, mix_bias, stream_count):
    scale_inv = lax.rsqrt(squares / (stream_count * D) + epsilon)
    logits = raw_logits * scale_inv[:, None] + mix_bias[None, :]
    pre_gate = jax.nn.sigmoid(logits[:, :stream_count])
    post_gate = 2.0 * jax.nn.sigmoid(logits[:, stream_count : 2 * stream_count])
    matrix = jnp.exp(logits[:, 2 * stream_count :]).reshape(-1, stream_count, stream_count)
    matrix = lax.fori_loop(0, ITERS, normalize, matrix)
    return (pre_gate, post_gate, matrix)


def contract_last(weights, rows):
    return lax.dot_general(
        weights, rows, (((1,), (1,)), ((), ())), preferred_element_type=jnp.float32
    )


def per_device(streams, mix_weight, mix_bias, gate_weight, up_weight, down_weight):
    tok_rows, stream_count, width_local = streams.shape
    logit_count = mix_weight.shape[0]
    flat_rows = streams.reshape(tok_rows, stream_count * width_local)
    flat_weight = mix_weight.reshape(logit_count, stream_count * width_local)
    raw_logits = lax.dot_general(
        flat_rows, flat_weight, (((1,), (1,)), ((), ())), preferred_element_type=jnp.float32
    )
    stream_wide = streams.astype(jnp.float32)
    squares = jnp.sum(stream_wide * stream_wide, axis=(1, 2))
    total_logits, total_squares = lax.psum((raw_logits, squares), "tensor")
    pre_gate, post_gate, res_mix = mixing(total_logits, total_squares, mix_bias, stream_count)
    mlp_input = jnp.einsum(
        "ts,tsc->tc", pre_gate, stream_wide, precision=lax.Precision.HIGHEST
    ).astype(jnp.bfloat16)
    unit_local = gate_weight.shape[0]
    block_rows = lax.all_gather(mlp_input, "dp", axis=0, tiled=True)
    gate_part = contract_last(gate_weight, block_rows)
    up_part = contract_last(up_weight, block_rows)
    both_parts = jnp.concatenate((gate_part, up_part), axis=0)
    unit_share = lax.psum_scatter(both_parts, "tensor", scatter_dimension=1, tiled=True)
    hidden_share = (jax.nn.silu(unit_share[:unit_local]) * unit_share[unit_local:]).astype(
        jnp.bfloat16
    )
    hidden = lax.all_gather(hidden_share, "tensor", axis=1, tiled=True)
    mlp_out = lax.psum_scatter(
        lax.dot_general(
            hidden, down_weight, (((0,), (0,)), ((), ())), preferred_element_type=jnp.float32
        ),
        "dp",
        scatter_dimension=0,
        tiled=True,
    )
    mixed = jnp.einsum("tij,tjc->tic", res_mix, stream_wide, precision=lax.Precision.HIGHEST)
    mixed = mixed + post_gate[:, :, None] * mlp_out[:, None, :]
    return mixed.astype(jnp.bfloat16)


MESH = pl.DeviceIdType.MESH
UNIT_CHUNK = 256
COLUMN_CHUNK = 256
PAIR = 2
GROUP = 3
D_LAG = 4
VMEM_BUDGET = 58 * 1024 * 1024


def column(values, at):
    return values[:, at : at + 1]


def sigmoid(v):
    return 1.0 / (1.0 + jnp.exp(-v))


def layer_kernel(
    plan,
    s_hbm,
    mw_hbm,
    bias_ref,
    gate_hbm,
    up_hbm,
    down_hbm,
    out_ref,
    gate_v,
    up_v,
    down_v,
    s_raw,
    mw_raw,
    s_ref,
    mw_ref,
    part,
    part_in,
    post,
    rows_all,
    mixed,
    sums,
    pair_in,
    pair_sum,
    ring_out,
    ring_in,
    hidden,
    prod,
    cross_out,
    cross_in,
    cross_sum,
    line_out,
    line_in,
    in_sem,
    w_sem,
    a_send,
    a_recv,
    bz_send,
    bz_recv,
    bx_send,
    bx_recv,
    c1_send,
    c1_recv,
    c2_send,
    c2_recv,
    c3_send,
    c3_recv,
    c4_send,
    c4_recv,
    d1_send,
    d1_recv,
    d2_send,
    d2_recv,
):
    zs, ys, tensors, chunks, nc, columns, cc, width_all = plan
    streams, tok, width = s_ref.shape
    dp = lax.axis_index("dp")
    tp = lax.axis_index("tensor")
    z, x = lax.div(dp, PAIR), lax.rem(dp, PAIR)
    y, core = lax.div(tp, PAIR), lax.rem(tp, PAIR)
    x_peer = (z * PAIR + 1 - x, tp)
    core_peer = (dp, y * PAIR + 1 - core)

    def z_at(r):
        return lax.rem(z + r + zs, zs)

    def y_at(r):
        return lax.rem(y + r + ys, ys)

    def z_peer(r):
        return (z_at(r) * PAIR + x, tp)

    def y_peer(r):
        return (dp, y_at(r) * PAIR + core)

    def t_peer(r):
        return (dp, lax.rem(tp + r, tensors))

    def send(src, dst, ssem, rsem, peer):
        return pltpu.make_async_remote_copy(
            src_ref=src, dst_ref=dst, send_sem=ssem, recv_sem=rsem, device_id=peer, device_id_type=MESH
        )

    def weight_copy(k, which):
        hbm, vmem = ((gate_hbm, gate_v), (up_hbm, up_v), (down_hbm, down_v))[which]
        return pltpu.make_async_copy(hbm.at[pl.ds(k * nc, nc)], vmem.at[pl.ds(k * nc, nc)], w_sem.at[which, k])

    def start_gate_up(k, _):
        weight_copy(k, 0).start()
        weight_copy(k, 1).start()
        return 0

    def start_down(k, _):
        weight_copy(k, 2).start()
        return 0

    barrier = pltpu.get_barrier_semaphore()
    peers = [t_peer(r) for r in range(1, tensors)] + [x_peer] + [z_peer(r) for r in range(1, zs)]
    for peer in peers:
        pl.semaphore_signal(barrier, inc=1, device_id=peer, device_id_type=MESH)

    inputs = (
        pltpu.make_async_copy(s_hbm, s_raw, in_sem.at[0]),
        pltpu.make_async_copy(mw_hbm, mw_raw, in_sem.at[1]),
    )
    for copy in inputs:
        copy.start()
    lax.fori_loop(0, chunks, start_gate_up, 0)
    lax.fori_loop(0, chunks, start_down, 0)
    for copy in inputs:
        copy.wait()
    for j in range(streams):
        s_ref[j] = s_raw[:, j, :]
        mw_ref[j] = mw_raw[:, j, :]

    raw = jnp.zeros((tok, mw_ref.shape[1]), jnp.float32)
    squares = jnp.zeros((tok, 1), jnp.float32)
    for j in range(streams):
        raw += contract_last(s_ref[j], mw_ref[j])
        wide = s_ref[j].astype(jnp.float32)
        squares += jnp.sum(wide * wide, axis=1, keepdims=True)
    count = raw.shape[1]
    part[...] = jnp.broadcast_to(squares, part.shape)
    part[:, :count] = raw
    pl.semaphore_wait(barrier, len(peers))

    def a_copy(r):
        return send(part, part_in.at[r - 1], a_send.at[r - 1], a_recv.at[r - 1], t_peer(r))

    for r in range(1, tensors):
        a_copy(r).start()
    for r in range(1, tensors):
        a_copy(r).wait_recv()
    total = part[...]
    for r in range(1, tensors):
        total = total + part_in[r - 1]
    scale_inv = lax.rsqrt(column(total, count) / width_all + epsilon)
    logits = total[:, :count] * scale_inv + bias_ref[...]
    gates = sigmoid(logits)
    mlp_input = column(gates, 0) * s_ref[0].astype(jnp.float32)
    for j in range(1, streams):
        mlp_input += column(gates, j) * s_ref[j].astype(jnp.float32)
    rows_all[z] = mlp_input.astype(jnp.bfloat16)

    def bz_copy(r):
        return send(rows_all.at[z], rows_all.at[z], bz_send.at[r - 1], bz_recv.at[r - 1], z_peer(r))

    def bx_copy(r):
        at = z_at(-r)
        return send(rows_all.at[at], rows_all.at[zs + at], bx_send.at[r], bx_recv.at[r], x_peer)

    bx_copy(0).start()
    for r in range(1, zs):
        bz_copy(r).start()
    for i in range(streams):
        post[i] = jnp.broadcast_to(2.0 * column(gates, streams + i), (tok, post.shape[2]))

    entries = jnp.exp(logits)
    mat = tuple(column(entries, 2 * streams + at) for at in range(streams * streams))

    def sweep(_, m):
        m = list(m)
        for i in range(streams):
            total_row = m[i * streams]
            for j in range(1, streams):
                total_row = total_row + m[i * streams + j]
            inv = 1.0 / total_row
            for j in range(streams):
                m[i * streams + j] = m[i * streams + j] * inv
        for j in range(streams):
            total_col = m[j]
            for i in range(1, streams):
                total_col = total_col + m[i * streams + j]
            inv = 1.0 / total_col
            for i in range(streams):
                m[i * streams + j] = m[i * streams + j] * inv
        return tuple(m)

    order = sorted(range(1, zs), key=lambda r: min(r, zs - r))
    share = ITERS // zs
    for r in order:
        mat = lax.fori_loop(0, share, sweep, mat)
        send(rows_all.at[z], rows_all.at[z_at(-r)], bz_send.at[r - 1], bz_recv.at[r - 1], z_peer(r)).wait_recv()
        bx_copy(r).start()
    mat = lax.fori_loop(0, ITERS - share * len(order), sweep, mat)
    for i in range(streams):
        line = mat[i * streams] * s_ref[0].astype(jnp.float32)
        for j in range(1, streams):
            line += mat[i * streams + j] * s_ref[j].astype(jnp.float32)
        mixed[i] = line

    def bx_arrival(r):
        at = z_at(-r)
        return send(rows_all.at[at], rows_all.at[zs + at], bx_send.at[r], bx_recv.at[r], x_peer)

    for r in range(zs):
        bx_arrival(r).wait_recv()

    prod[...] = jnp.zeros_like(prod)
    group = GROUP if chunks % GROUP == 0 else 1

    tokens = PAIR * zs * tok
    half = tokens // PAIR
    quarter = half // ys
    own_slot = core * ys + y

    def c1_copy(k):
        return send(sums.at[k, 1 - core], pair_in.at[k], c1_send.at[k], c1_recv.at[k], core_peer)

    def c2_copy(k, r):
        at = (k * (ys - 1)) + r - 1
        return send(ring_out.at[at], ring_in.at[at], c2_send.at[at], c2_recv.at[at], y_peer(r))

    def units(k):
        return pl.ds(pl.multiple_of(k * nc, nc), nc)

    def c3_copy(k, r):
        at = (k * (ys - 1)) + r - 1
        piece = hidden.at[own_slot, :, units(k)]
        return send(piece, piece, c3_send.at[at], c3_recv.at[at], y_peer(r))

    def c3_arrival(k, r):
        at = (k * (ys - 1)) + r - 1
        piece = hidden.at[core * ys + y_at(-r), :, units(k)]
        return send(piece, piece, c3_send.at[at], c3_recv.at[at], y_peer(r))

    def c4_copy(k, r):
        at = k * ys + r
        piece = hidden.at[core * ys + y_at(-r), :, units(k)]
        return send(piece, piece, c4_send.at[at], c4_recv.at[at], core_peer)

    def c4_arrival(k, r):
        at = k * ys + r
        piece = hidden.at[(1 - core) * ys + y_at(-r), :, units(k)]
        return send(piece, piece, c4_send.at[at], c4_recv.at[at], core_peer)

    def c_first(k):
        weight_copy(k, 0).wait()
        weight_copy(k, 1).wait()
        rows = rows_all[...].reshape(tokens, width)
        sums[k, :, :, :nc] = contract_last(rows, gate_v[pl.ds(k * nc, nc)]).reshape(PAIR, half, nc)
        sums[k, :, :, nc:] = contract_last(rows, up_v[pl.ds(k * nc, nc)]).reshape(PAIR, half, nc)
        c1_copy(k).start()

    def c_second(k):
        c1_copy(k).wait_recv()
        both = sums[k, core] + pair_in[k]
        pair_sum[k] = both.reshape(ys, quarter, PAIR * nc)
        for r in range(1, ys):
            ring_out[k * (ys - 1) + r - 1] = pair_sum[k, y_at(r)].astype(jnp.bfloat16)
            c2_copy(k, r).start()

    def c_third(k):
        both = pair_sum[k, y]
        for r in range(1, ys):
            c2_copy(k, r).wait_recv()
            both = both + ring_in[k * (ys - 1) + r - 1].astype(jnp.float32)
        gate, up = both[:, :nc], both[:, nc:]
        hidden[own_slot, :, units(k)] = (gate / (1.0 + jnp.exp(-gate)) * up).astype(jnp.bfloat16)
        for r in range(1, ys):
            c3_copy(k, r).start()
        c4_copy(k, 0).start()

    def c_fourth(k):
        for r in range(1, ys):
            c3_arrival(k, r).wait_recv()
            c4_copy(k, r).start()

    def pipeline(count, stages):
        last = max(lag for lag, _ in stages)

        def step(t, _):
            for lag, stage in stages:
                @pl.when(jnp.logical_and(t >= lag, t < count + lag))
                def _():
                    stage(t - lag)

            return 0

        lax.fori_loop(0, count + last, step, 0)

    def cols(n):
        return pl.ds(pl.multiple_of(n * cc, cc), cc)

    def down_piece(first, n):
        span = pl.ds(pl.multiple_of(first * nc, nc), group * nc)
        rows = hidden[:, :, span].reshape(tokens, group * nc)
        return jnp.dot(rows, down_v[span, cols(n)], preferred_element_type=jnp.float32)

    def c_fifth(k):
        for r in range(ys):
            c4_arrival(k, r).wait_recv()
        weight_copy(k, 2).wait()

        @pl.when(jnp.logical_and(lax.rem(k, group) == group - 1, k < chunks - group))
        def _():
            def add(n, _):
                prod[n] = prod[n] + down_piece(k - (group - 1), n)
                return 0

            lax.fori_loop(0, columns, add, 0)

    pipeline(chunks, ((0, c_first), (2, c_second), (5, c_third), (8, c_fourth), (10, c_fifth)))

    def d1_copy(n):
        return send(cross_out.at[n], cross_in.at[n], d1_send.at[n], d1_recv.at[n], x_peer)

    def d2_copy(n, r):
        at = n * (zs - 1) + r - 1
        return send(line_out.at[at], line_in.at[at], d2_send.at[at], d2_recv.at[at], z_peer(r))

    def d_first(n):
        product = prod[n] + down_piece(chunks - group, n)
        prod[n, :half] = product[:half]
        cross_out[n] = product[half:].astype(jnp.bfloat16)
        d1_copy(n).start()

    def d_second(n):
        d1_copy(n).wait_recv()
        cross_sum[n] = (prod[n, :half] + cross_in[n].astype(jnp.float32)).reshape(zs, tok, cc)
        for r in range(1, zs):
            line_out[n * (zs - 1) + r - 1] = cross_sum[n, z_at(r)].astype(jnp.bfloat16)
            d2_copy(n, r).start()

    def d_third(n):
        mlp_out = cross_sum[n, z]
        for r in range(1, zs):
            d2_copy(n, r).wait_recv()
            mlp_out = mlp_out + line_in[n * (zs - 1) + r - 1].astype(jnp.float32)
        for i in range(streams):
            out_ref[i, :, cols(n)] = (mixed[i, :, cols(n)] + column(post[i], 0) * mlp_out).astype(jnp.bfloat16)

    pipeline(columns, ((0, d_first), (D_LAG, d_second), (2 * D_LAG, d_third)))

    for r in range(1, tensors):
        a_copy(r).wait_send()
    for r in range(1, zs):
        bz_copy(r).wait_send()
    for r in range(zs):
        bx_copy(r).wait_send()

    def drain_c(k, _):
        c1_copy(k).wait_send()
        for r in range(1, ys):
            c2_copy(k, r).wait_send()
            c3_copy(k, r).wait_send()
        for r in range(ys):
            c4_copy(k, r).wait_send()
        return 0

    def drain_d(n, _):
        d1_copy(n).wait_send()
        for r in range(1, zs):
            d2_copy(n, r).wait_send()
        return 0

    lax.fori_loop(0, chunks, drain_c, 0)
    lax.fori_loop(0, columns, drain_d, 0)


def layer_scratch(zs, ys, tensors, tok, streams, logits, width, units, nc, cc):
    tokens = PAIR * zs * tok
    half = tokens // PAIR
    quarter = half // ys
    chunks, columns = units // nc, width // cc
    f32, bf16 = jnp.float32, jnp.bfloat16
    lanes = 128
    arrays = [
        ((units, width), bf16),
        ((units, width), bf16),
        ((units, width), bf16),
        ((tok, streams, width), bf16),
        ((logits, streams, width), bf16),
        ((streams, tok, width), bf16),
        ((streams, logits, width), bf16),
        ((tok, lanes), f32),
        ((tensors - 1, tok, lanes), f32),
        ((streams, tok, lanes), f32),
        ((PAIR * zs, tok, width), bf16),
        ((streams, tok, width), f32),
        ((chunks, PAIR, half, 2 * nc), f32),
        ((chunks, half, 2 * nc), f32),
        ((chunks, ys, quarter, 2 * nc), f32),
        ((chunks * (ys - 1), quarter, 2 * nc), bf16),
        ((chunks * (ys - 1), quarter, 2 * nc), bf16),
        ((PAIR * ys, quarter, units), bf16),
        ((columns, tokens, cc), f32),
        ((columns, half, cc), bf16),
        ((columns, half, cc), bf16),
        ((columns, zs, tok, cc), f32),
        ((columns * (zs - 1), tok, cc), bf16),
        ((columns * (zs - 1), tok, cc), bf16),
    ]
    both = lambda count: [(count,), (count,)]
    sems = [(2,), (3, chunks)]
    for count in (tensors - 1, zs - 1, zs, chunks, chunks * (ys - 1), chunks * (ys - 1), chunks * ys, columns, columns * (zs - 1)):
        sems += both(count)
    size = sum(math.prod(shape) * jnp.dtype(kind).itemsize for shape, kind in arrays)
    return arrays, sems, size


def fused(mesh, streams, mix_weight, mix_bias, gate_weight, up_weight, down_weight):
    tok, stream_count, width = streams.shape
    units = gate_weight.shape[0]
    dps, tensors = mesh.shape["dp"], mesh.shape["tensor"]
    zs, ys = dps // PAIR, tensors // PAIR
    nc, cc = UNIT_CHUNK, COLUMN_CHUNK
    arrays, sems, _ = layer_scratch(zs, ys, tensors, tok, stream_count, mix_weight.shape[0], width, units, nc, cc)
    plan = (zs, ys, tensors, units // nc, nc, width // cc, cc, stream_count * width * tensors)
    bias = mix_bias[None, :]
    vmem = pl.BlockSpec(memory_space=pltpu.VMEM)
    hbm = pl.BlockSpec(memory_space=pl.ANY)
    out = pl.pallas_call(
        functools.partial(layer_kernel, plan),
        out_shape=jax.ShapeDtypeStruct((stream_count, tok, width), jnp.bfloat16),
        in_specs=[hbm, hbm, vmem, hbm, hbm, hbm],
        out_specs=vmem,
        scratch_shapes=[pltpu.VMEM(shape, kind) for shape, kind in arrays]
        + [pltpu.SemaphoreType.DMA(shape) for shape in sems],
        compiler_params=pltpu.CompilerParams(
            collective_id=0, has_side_effects=True, vmem_limit_bytes=VMEM_BUDGET
        ),
    )(streams, mix_weight, bias, gate_weight, up_weight, down_weight)
    return out.transpose(1, 0, 2)


def fits(mesh, streams, mix_weight, gate_weight):
    tok, stream_count, width = streams.shape
    units = gate_weight.shape[0]
    dps, tensors = mesh.shape["dp"], mesh.shape["tensor"]
    if dps % PAIR or tensors % PAIR or dps < 2 * PAIR or tensors < 2 * PAIR:
        return False
    zs, ys = dps // PAIR, tensors // PAIR
    if units % UNIT_CHUNK or width % COLUMN_CHUNK or tok % 16 or (zs * tok) % (16 * ys):
        return False
    if mix_weight.shape[0] >= 128:
        return False
    size = layer_scratch(
        zs, ys, tensors, tok, stream_count, mix_weight.shape[0], width, units, UNIT_CHUNK, COLUMN_CHUNK
    )[2]
    return size < VMEM_BUDGET * 3 // 4


def solution(mesh):
    in_specs = (
        P("dp", None, "tensor"),
        P(None, None, "tensor"),
        P(),
        P("dp", "tensor"),
        P("dp", "tensor"),
        P("dp", "tensor"),
    )
    out_specs = P("dp", None, "tensor")

    def step(streams, mix_weight, mix_bias, gate_weight, up_weight, down_weight):
        operands = (streams, mix_weight, mix_bias, gate_weight, up_weight, down_weight)
        if fits(mesh, streams, mix_weight, gate_weight):
            return fused(mesh, *operands)
        return per_device(*operands)

    return jax.shard_map(step, mesh=mesh, in_specs=in_specs, out_specs=out_specs, check_vma=False)
```
